32 devices in a mesh: seq: 8 (over z, core), fsdp: 4 (over y, x).
Axes of the slice: x: 2, y: 2, z: 4, core: 2. Of those that a mesh axis runs over, the one named last changes fastest.
Arguments:
- block_input: bfloat16 [8, 1472, 1152], P('fsdp', 'seq')
- key_mask: int32 [16, 736], P('fsdp'), may hold values from 0 to 1, as said below
- slot_flags: int32 [16], P('fsdp'), may hold values from 0 to 1, as said below
- norm1_gain: bfloat16 [1152], P('fsdp'), may hold values from 0.5 to 1.5
- norm1_bias: bfloat16 [1152], P('fsdp'), may hold values from -3 to 3
- qkv_weight: bfloat16 [1152, 3456], P('fsdp'), may hold values from -0.25 to 0.25
- query_bias: bfloat16 [1152], P('fsdp'), may hold values from -3 to 3
- value_bias: bfloat16 [1152], P('fsdp'), may hold values from -3 to 3
- proj_weight: bfloat16 [1152, 1152], P('fsdp'), may hold values from -0.375 to 0.375
- proj_bias: bfloat16 [1152], P('fsdp'), may hold values from -3 to 3
- norm2_gain: bfloat16 [1152], P('fsdp'), may hold values from 0.5 to 1.5
- norm2_bias: bfloat16 [1152], P('fsdp'), may hold values from -3 to 3
- up_weight: bfloat16 [1152, 4304], P('fsdp'), may hold values from -0.1875 to 0.1875
- up_bias: bfloat16 [4304], P('fsdp'), may hold values from -3 to 3
- down_weight: bfloat16 [4304, 1152], P(None, 'fsdp'), may hold values from -0.09375 to 0.09375
- down_bias: bfloat16 [1152], P('fsdp'), may hold values from -3 to 3
- out_grad: bfloat16 [8, 1472, 1152], P('fsdp', 'seq'), may hold values from -6 to 6
Outputs:
- block_output: bfloat16 [8, 1472, 1152], P('fsdp', 'seq')
- input_grad: float32 [8, 1472, 1152], P('fsdp', 'seq')
- norm1_gain_grad: float32 [1152], P('fsdp')
- norm1_bias_grad: float32 [1152], P('fsdp')
- qkv_weight_grad: float32 [1152, 3456], P('fsdp')
- query_bias_grad: float32 [1152], P('fsdp')
- value_bias_grad: float32 [1152], P('fsdp')
- proj_weight_grad: float32 [1152, 1152], P('fsdp')
- proj_bias_grad: float32 [1152], P('fsdp')
- norm2_gain_grad: float32 [1152], P('fsdp')
- norm2_bias_grad: float32 [1152], P('fsdp')
- up_weight_grad: float32 [1152, 4304], P('fsdp')
- up_bias_grad: float32 [4304], P('fsdp')
- down_weight_grad: float32 [4304, 1152], P(None, 'fsdp')
- down_bias_grad: float32 [1152], P('fsdp')
The draws below stay inside these ranges and needn't reach their ends.
Inputs may be any that keep to these rules, and one draw needn't show every extreme that they name: `key_mask`: positions 729 and beyond are 0 in every slot; every position of a slot whose flag is 0 is 0. `slot_flags`: exactly max(1, 1) slots have flag 0, at places drawn from the seed.
All inputs are finite; a program needn't handle non-finite values.
Results may differ from the reference program's by a relative error of at most 0.012.
The reference program's roundings to bfloat16 on the way count: a program that leaves them out, or rounds other values in their place, can miss the bound.
Values may be sent and summed in bfloat16 or wider, within the bound.
A program may use at most 256 MiB of HBM per device.

```python
import math
import jax
import jax.numpy as jnp
from jax import lax

D = 1152
HEADS = 16
HEAD = 72
FF = 4304
PATCHES = 729
SLOT = 736
IMAGES = 16


def slot_layout(key):
    folded = jax.random.fold_in(key, 7)
    shuffled = jax.random.permutation(jax.random.fold_in(folded, 1), IMAGES)
    fake_count = max(1, IMAGES * 7 // 96)
    slot_live = (shuffled >= fake_count).astype(jnp.int32)
    draws_int = jax.random.randint(jax.random.fold_in(folded, 2), (IMAGES, SLOT), 0, 10)
    places = jnp.arange(SLOT)[None, :]
    key_live = ((draws_int > 0) & (places < PATCHES)).astype(jnp.int32) * slot_live[:, None]
    return (slot_live, key_live)


def draw_key_mask(key, part):
    return slot_layout(key)[1]


def draw_slot_flags(key, part):
    return slot_layout(key)[0]


def draw_block_input(key, part):
    row_scale = jnp.exp(jax.random.uniform(jax.random.fold_in(key, 12), (IMAGES, SLOT, 1), jnp.float32, -1.15, 1.15))
    col_scale = jnp.exp(jax.random.uniform(jax.random.fold_in(key, 13), (1, 1, D), jnp.float32, -1.15, 1.15))
    values = jax.random.normal(jax.random.fold_in(key, 11), (IMAGES, SLOT, D), jnp.float32) * row_scale * col_scale
    return values.reshape(IMAGES // 2, 2 * SLOT, D).astype(jnp.bfloat16)


def levels(stream_key, shape, pieces, low, largest):
    def one(axis_at, blocks):
        heights = jax.random.uniform(jax.random.fold_in(jax.random.fold_in(stream_key, 6), axis_at), (blocks,), jnp.float32, low / len(pieces), largest / len(pieces))
        return jnp.repeat(jnp.exp(heights), shape[axis_at] // blocks).reshape((-1,) + (1,) * (len(shape) - axis_at - 1))

    loudness = one(*pieces[0])
    for cut in pieces[1:]:
        loudness = loudness * one(*cut)
    return loudness


def gaussian(own_key, extent, scale, bound, cuts=(), held_as=jnp.bfloat16):
    drawn = jax.random.normal(own_key, extent, jnp.float32) * scale
    if len(cuts) > 0:
        drawn = levels(own_key, extent, cuts, -0.22, 0.18) * drawn
    return jnp.clip(drawn, min=-bound, max=bound).astype(held_as)


def setup_inputs(seed: int = 0) -> dict:
    seeds = jax.random.split(jax.random.key(seed), 18)
    block_input = draw_block_input(jax.random.fold_in(seeds[17], 71), 0)
    key_mask = draw_key_mask(jax.random.fold_in(seeds[17], 71), 0)
    slot_flags = draw_slot_flags(jax.random.fold_in(seeds[17], 71), 0)
    norm1_gain = jnp.clip(1.0 + 0.1 * jax.random.normal(seeds[3], (D,), jnp.float32), 0.5, 1.5).astype(jnp.bfloat16)
    norm1_bias = gaussian(seeds[4], (D,), 0.5, 3.0, ((0, 4),))
    qkv_weight = gaussian(seeds[5], (D, 3 * D), (D // 2) ** -0.5, 0.25, ((0, 4),))
    query_bias = gaussian(seeds[6], (D,), 0.5, 3.0, ((0, 4),))
    value_bias = gaussian(seeds[7], (D,), 0.5, 3.0, ((0, 4),))
    proj_weight = gaussian(seeds[8], (D, D), (D // 4) ** -0.5, 0.375, ((0, 4),))
    proj_bias = gaussian(seeds[9], (D,), 0.5, 3.0, ((0, 4),))
    norm2_gain = jnp.clip(1.0 + 0.1 * jax.random.normal(seeds[10], (D,), jnp.float32), 0.5, 1.5).astype(jnp.bfloat16)
    norm2_bias = gaussian(seeds[11], (D,), 0.5, 3.0, ((0, 4),))
    up_weight = gaussian(seeds[12], (D, FF), D ** -0.5, 0.1875, ((0, 4),))
    up_bias = gaussian(seeds[13], (FF,), 0.5, 3.0, ((0, 4),))
    down_weight = gaussian(seeds[14], (FF, D), FF ** -0.5, 0.09375, ((1, 4),))
    down_bias = gaussian(seeds[15], (D,), 0.5, 3.0, ((0, 4),))
    out_grad = gaussian(seeds[16], (IMAGES // 2, 2 * SLOT, D), 1.0, 6.0, ((0, 4), (1, 8)))
    return dict(block_input=block_input, key_mask=key_mask, slot_flags=slot_flags, norm1_gain=norm1_gain, norm1_bias=norm1_bias, qkv_weight=qkv_weight, query_bias=query_bias, value_bias=value_bias, proj_weight=proj_weight, proj_bias=proj_bias, norm2_gain=norm2_gain, norm2_bias=norm2_bias, up_weight=up_weight, up_bias=up_bias, down_weight=down_weight, down_bias=down_bias, out_grad=out_grad)


epsilon = 1e-06
precise = lax.Precision.HIGHEST

@jax.custom_vjp
def low(v):
    return lax.optimization_barrier(v.astype(jnp.bfloat16)).astype(jnp.float32)

@jax.custom_vjp
def low_back(v):
    return v

def low_keep(v):
    return (low(v), None)

def low_pass(kept, grad):
    return (grad,)

def back_keep(v):
    return (v, None)

def back_low(kept, grad):
    return (low(grad),)
low.defvjp(low_keep, low_pass)
low_back.defvjp(back_keep, back_low)

def layer_norm(values, gain_vec, bias_vec):
    row_mean = lax.optimization_barrier(jnp.mean(values, axis=-1, keepdims=True))
    centered = values - row_mean
    variance = lax.optimization_barrier(jnp.mean(centered * centered, axis=-1, keepdims=True))
    return centered * lax.rsqrt(variance + epsilon) * gain_vec + bias_vec

def gelu_tanh(values):
    return 0.5 * values * (1.0 + jnp.tanh(0.7978845608028654 * (values + 0.044715 * values * values * values)))

def attend_slot(packed):
    queries, key_vecs, value_vecs, key_live = packed
    scores = low_back(jnp.einsum('qhd,khd->hqk', queries, key_vecs, precision=precise) * HEAD ** (-0.5))
    shifted = scores + ((key_live.astype(jnp.float32) - 1.0) * 10000.0)[None, None, :]
    row_max = lax.optimization_barrier(jnp.max(shifted, axis=-1, keepdims=True))
    exp_terms = jnp.exp(shifted - row_max)
    weights_low = low(exp_terms / lax.optimization_barrier(jnp.sum(exp_terms, axis=-1, keepdims=True)))
    return jnp.einsum('hqk,khd->qhd', weights_low, value_vecs, precision=precise)

def block_forward(inputs, live_part, flag_part, params):
    gain_one, bias_one, qkv_full, query_shift, value_shift, proj_full, proj_shift, gain_two, bias_two, up_full, up_shift, down_full, down_shift = params
    slot_count = inputs.shape[0]
    token_rows = inputs.reshape(slot_count * SLOT, D)
    normed = low(layer_norm(token_rows, gain_one, bias_one))
    mixed_rows = jnp.dot(normed, qkv_full, precision=precise)
    queries = low(low_back(mixed_rows[:, :D] + query_shift))
    key_vecs = low(low_back(mixed_rows[:, D:2 * D]))
    value_vecs = low(low_back(mixed_rows[:, 2 * D:] + value_shift))
    head_shape = (slot_count, SLOT, HEADS, HEAD)
    attended = lax.map(jax.checkpoint(attend_slot), (queries.reshape(head_shape), key_vecs.reshape(head_shape), value_vecs.reshape(head_shape), live_part))
    merged = low(low_back(attended.reshape(slot_count * SLOT, D)))
    branch = low_back(jnp.dot(merged, proj_full, precision=precise) + proj_shift)
    hidden = token_rows + branch
    second = low(layer_norm(hidden, gain_two, bias_two))
    gate_in = low_back(jnp.dot(second, up_full, precision=precise) + up_shift)
    active = low(gelu_tanh(gate_in))
    result = hidden + low_back(jnp.dot(active, down_full, precision=precise) + down_shift)
    return result.reshape(slot_count, SLOT, D) * flag_part.astype(jnp.float32)[:, None, None]

def reference(block_input, key_mask, slot_flags, norm1_gain, norm1_bias, qkv_weight, query_bias, value_bias, proj_weight, proj_bias, norm2_gain, norm2_bias, up_weight, up_bias, down_weight, down_bias, out_grad):
    params = tuple((p.astype(jnp.float32) for p in (norm1_gain, norm1_bias, qkv_weight, query_bias, value_bias, proj_weight, proj_bias, norm2_gain, norm2_bias, up_weight, up_bias, down_weight, down_bias)))
    per_step = math.gcd(IMAGES, 4)
    step_count = IMAGES // per_step
    inputs = block_input.reshape(step_count, per_step, SLOT, D)
    live_groups = key_mask.reshape(step_count, per_step, SLOT)
    flag_groups = slot_flags.reshape(step_count, per_step)
    cot_groups = out_grad.reshape(step_count, per_step, SLOT, D)

    def scan_step(running, batch_part):
        inputs_part, live_part, flag_part, grad_part = batch_part
        outputs, pullback = jax.vjp(lambda a, b: block_forward(a, live_part, flag_part, b), inputs_part.astype(jnp.float32), params)
        grad_input, grad_params = pullback(grad_part.astype(jnp.float32))
        running = jax.tree.map(lambda a, b: a + b, running, grad_params)
        return (running, (outputs.astype(jnp.bfloat16), grad_input))
    zero_grads = jax.tree.map(jnp.zeros_like, params)
    totals, (outputs, grad_inputs) = lax.scan(scan_step, zero_grads, (inputs, live_groups, flag_groups, cot_groups))
    pair_shape = (IMAGES // 2, 2 * SLOT, D)
    return (outputs.reshape(pair_shape), grad_inputs.reshape(pair_shape), totals[0], totals[1], totals[2], totals[3], totals[4], totals[5], totals[6], totals[7], totals[8], totals[9], totals[10], totals[11], totals[12])
```

```python
import jax
import jax.numpy as jnp
from jax import lax
from jax.sharding import Mesh
from jax.sharding import PartitionSpec as P

HEADS = 16
HEAD = 72
epsilon = 1e-06

SEQ = ("zh", "zl", "core")
ZAX = ("zh", "zl")
GROUP = ("zl", "core")


def layer_norm(values, gain_vec, bias_vec):
    row_mean = jnp.mean(values, axis=-1, keepdims=True)
    centered = values - row_mean
    variance = jnp.mean(centered * centered, axis=-1, keepdims=True)
    return centered * lax.rsqrt(variance + epsilon) * gain_vec + bias_vec


def gelu_tanh(values):
    return (
        0.5
        * values
        * (1.0 + jnp.tanh(0.7978845608028654 * (values + 0.044715 * values * values * values)))
    )


def gather_weight(w, axis):
    half = w.shape[axis] // 2
    core = lax.axis_index("core")
    piece = lax.dynamic_slice_in_dim(w, core * half, half, axis=axis)
    return lax.all_gather(piece, ("fsdp", "core"), axis=axis, tiled=True)


def reduce_weight(g, axis):
    part = lax.psum_scatter(
        g.astype(jnp.bfloat16), ("fsdp", "core"), scatter_dimension=axis, tiled=True
    )
    part = lax.psum(part.astype(jnp.float32), ZAX)
    return lax.all_gather(part, "core", axis=axis, tiled=True)


def shards(
    block_input,
    key_mask,
    slot_flags,
    norm1_gain,
    norm1_bias,
    qkv_weight,
    query_bias,
    value_bias,
    proj_weight,
    proj_bias,
    norm2_gain,
    norm2_bias,
    up_weight,
    up_bias,
    down_weight,
    down_bias,
    out_grad,
):
    f32, bf16 = jnp.float32, jnp.bfloat16
    pairs, part_rows, width = block_input.shape
    group = lax.axis_size("zl") * lax.axis_size("core")
    local_heads = HEADS // group
    slot_len = part_rows * group
    zh = lax.axis_index("zh")
    scale = HEAD ** (-0.5)

    vectors = (norm1_gain, norm1_bias, query_bias, value_bias, proj_bias, norm2_gain,
               norm2_bias, up_bias, down_bias)
    sizes = [v.shape[0] for v in vectors]
    packed = jnp.concatenate([v.astype(f32) for v in vectors])
    packed = lax.all_gather(packed, "fsdp", axis=0, tiled=False)
    full_vectors = []
    at = 0
    for n in sizes:
        full_vectors.append(packed[:, at : at + n].reshape(-1))
        at += n
    g1, b1, bq, bv, bproj, g2, b2, bup, bdown = full_vectors

    w_qkv = gather_weight(qkv_weight, 0)
    w_proj = gather_weight(proj_weight, 0)
    w_up = gather_weight(up_weight, 0)
    w_down = gather_weight(down_weight, 1)

    flags = slot_flags.astype(f32).reshape(pairs, 2)
    row_flags = lax.dynamic_index_in_dim(flags, zh, axis=1, keepdims=False)
    live = lax.dynamic_index_in_dim(key_mask.reshape(pairs, 2, -1), zh, axis=1, keepdims=False)
    mask_bias = (live.astype(f32) - 1.0) * 10000.0

    rows = block_input.reshape(pairs * part_rows, width).astype(f32)
    normed, norm_one_back = jax.vjp(layer_norm, rows, g1, b1)
    normed_low = normed.astype(bf16)
    mixed = jnp.dot(normed_low, w_qkv, preferred_element_type=f32)
    q = (mixed[:, :width] + bq).astype(bf16)
    k = mixed[:, width : 2 * width].astype(bf16)
    v = (mixed[:, 2 * width :] + bv).astype(bf16)
    qkv_tok = jnp.stack([q, k, v]).reshape(3, pairs, part_rows, width)
    qkv_heads = lax.all_to_all(qkv_tok, GROUP, split_axis=3, concat_axis=2, tiled=True)
    qkv_heads = qkv_heads.reshape(3, pairs, slot_len, local_heads, HEAD)
    qh, kh, vh = qkv_heads[0], qkv_heads[1], qkv_heads[2]

    scores = jnp.einsum("pqhd,pkhd->phqk", qh, kh, preferred_element_type=f32) * scale
    shifted = scores + mask_bias[:, None, None, :]
    row_max = jnp.max(shifted, axis=-1, keepdims=True)
    exp_terms = jnp.exp(shifted - row_max)
    probs = exp_terms / jnp.sum(exp_terms, axis=-1, keepdims=True)
    weights_low = probs.astype(bf16)
    attended = jnp.einsum("phqk,pkhd->pqhd", weights_low, vh, preferred_element_type=f32)
    attended = attended.astype(bf16).reshape(pairs, slot_len, local_heads * HEAD)
    merged = lax.all_to_all(attended, GROUP, split_axis=1, concat_axis=2, tiled=True)
    merged_rows = merged.reshape(pairs * part_rows, width)

    hidden = rows + jnp.dot(merged_rows, w_proj, preferred_element_type=f32) + bproj
    second, norm_two_back = jax.vjp(layer_norm, hidden, g2, b2)
    second_low = second.astype(bf16)
    gate_in = jnp.dot(second_low, w_up, preferred_element_type=f32) + bup
    active, gelu_back = jax.vjp(gelu_tanh, gate_in)
    active_low = active.astype(bf16)
    result = hidden + jnp.dot(active_low, w_down, preferred_element_type=f32) + bdown
    row_flag_rows = jnp.repeat(row_flags, part_rows)[:, None]
    output = (result * row_flag_rows).astype(bf16).reshape(pairs, part_rows, width)

    grad_rows = out_grad.reshape(pairs * part_rows, width).astype(f32) * row_flag_rows
    grad_low = grad_rows.astype(bf16)
    down_weight_grad = jnp.dot(active_low.T, grad_low, preferred_element_type=f32)
    down_bias_grad = jnp.sum(grad_rows, axis=0)
    grad_active = jnp.dot(grad_low, w_down.T, preferred_element_type=f32)
    grad_gate = gelu_back(grad_active)[0].astype(bf16)
    up_weight_grad = jnp.dot(second_low.T, grad_gate, preferred_element_type=f32)
    up_bias_grad = jnp.sum(grad_gate.astype(f32), axis=0)
    grad_second = jnp.dot(grad_gate, w_up.T, preferred_element_type=f32)
    grad_hidden_norm, norm2_gain_grad, norm2_bias_grad = norm_two_back(grad_second)
    grad_hidden = grad_rows + grad_hidden_norm
    grad_branch = grad_hidden.astype(bf16)
    proj_weight_grad = jnp.dot(merged_rows.T, grad_branch, preferred_element_type=f32)
    proj_bias_grad = jnp.sum(grad_branch.astype(f32), axis=0)
    grad_merged = jnp.dot(grad_branch, w_proj.T, preferred_element_type=f32).astype(bf16)
    grad_heads = lax.all_to_all(
        grad_merged.reshape(pairs, part_rows, width), GROUP, split_axis=2, concat_axis=1, tiled=True
    ).reshape(pairs, slot_len, local_heads, HEAD)

    grad_probs = jnp.einsum("pqhd,pkhd->phqk", grad_heads, vh, preferred_element_type=f32)
    row_dot = jnp.sum(probs * grad_probs, axis=-1, keepdims=True)
    grad_scores = (probs * (grad_probs - row_dot)).astype(bf16)
    dq = (jnp.einsum("phqk,pkhd->pqhd", grad_scores, kh, preferred_element_type=f32) * scale).astype(bf16)
    dk = (jnp.einsum("phqk,pqhd->pkhd", grad_scores, qh, preferred_element_type=f32) * scale).astype(bf16)
    dv = jnp.einsum("phqk,pqhd->pkhd", weights_low, grad_heads, preferred_element_type=f32).astype(bf16)
    dqkv = jnp.stack([dq, dk, dv]).reshape(3, pairs, slot_len, local_heads * HEAD)
    dqkv_tok = lax.all_to_all(dqkv, GROUP, split_axis=2, concat_axis=3, tiled=True)
    dqkv_tok = dqkv_tok.reshape(3, pairs * part_rows, width)
    grad_mixed = jnp.concatenate([dqkv_tok[0], dqkv_tok[1], dqkv_tok[2]], axis=1)
    qkv_weight_grad = jnp.dot(normed_low.T, grad_mixed, preferred_element_type=f32)
    query_bias_grad = jnp.sum(dqkv_tok[0].astype(f32), axis=0)
    value_bias_grad = jnp.sum(dqkv_tok[2].astype(f32), axis=0)
    grad_normed = jnp.dot(grad_mixed, w_qkv.T, preferred_element_type=f32)
    grad_rows_norm, norm1_gain_grad, norm1_bias_grad = norm_one_back(grad_normed)
    input_grad = (grad_hidden + grad_rows_norm).reshape(pairs, part_rows, width)

    vec_grads = (norm1_gain_grad, norm1_bias_grad, query_bias_grad, value_bias_grad,
                 proj_bias_grad, norm2_gain_grad, norm2_bias_grad, up_bias_grad, down_bias_grad)
    fsdp = lax.axis_size("fsdp")
    stacked = jnp.concatenate([g.reshape(fsdp, -1) for g in vec_grads], axis=1)
    stacked = lax.psum_scatter(stacked, "fsdp", scatter_dimension=0, tiled=True)
    stacked = lax.psum(stacked, SEQ).reshape(-1)
    vec_out = []
    at = 0
    for g in vec_grads:
        n = g.shape[0] // fsdp
        vec_out.append(stacked[at : at + n])
        at += n
    (n1g, n1b, qb, vb, pb, n2g, n2b, ub, db) = vec_out

    qkv_g = reduce_weight(qkv_weight_grad, 0)
    proj_g = reduce_weight(proj_weight_grad, 0)
    up_g = reduce_weight(up_weight_grad, 0)
    down_g = reduce_weight(down_weight_grad, 1)

    return (output, input_grad, n1g, n1b, qkv_g, qb, vb, proj_g, pb, n2g, n2b, up_g, ub, down_g, db)


def solution(mesh):
    seq_n = mesh.shape["seq"]
    fsdp_n = mesh.shape["fsdp"]
    devices = mesh.devices.reshape(2, seq_n // 4, 2, fsdp_n)
    inner = Mesh(devices, ("zh", "zl", "core", "fsdp"))
    tok = P("fsdp", SEQ, None)
    vec = P("fsdp")
    rows = P("fsdp", None)
    in_specs = (tok, rows, vec, vec, vec, rows, vec, vec, rows, vec, vec, vec, rows, vec,
                P(None, "fsdp"), vec, tok)
    out_specs = (tok, tok, vec, vec, rows, vec, vec, rows, vec, vec, vec, rows, vec,
                 P(None, "fsdp"), vec)
    return jax.shard_map(shards, mesh=inner, in_specs=in_specs, out_specs=out_specs, check_vma=False)
```

```python
import jax
import jax.numpy as jnp
from jax import lax
from jax.sharding import Mesh
from jax.sharding import PartitionSpec as P

HEADS = 16
HEAD = 72
epsilon = 1e-06

SEQ = ("zh", "zl", "core")
ZAX = ("zh", "zl")
GROUP = ("zl", "core")


def layer_norm(values, gain_vec, bias_vec):
    row_mean = jnp.mean(values, axis=-1, keepdims=True)
    centered = values - row_mean
    variance = jnp.mean(centered * centered, axis=-1, keepdims=True)
    return centered * lax.rsqrt(variance + epsilon) * gain_vec + bias_vec


def gelu_tanh(values):
    return (
        0.5
        * values
        * (1.0 + jnp.tanh(0.7978845608028654 * (values + 0.044715 * values * values * values)))
    )


def core_swap(x):
    return lax.ppermute(x, "core", [(0, 1), (1, 0)])


def in_core_order(mine, other):
    first = lax.axis_index("core") == 0
    return jnp.where(first, mine, other), jnp.where(first, other, mine)


def gather_weight(w):
    rows, cols = w.shape
    half = rows // 2
    piece = lax.dynamic_slice_in_dim(w, lax.axis_index("core") * half, half, axis=0)
    mine = lax.all_gather(piece, "fsdp", axis=0, tiled=False)
    other = core_swap(mine)
    first, second = in_core_order(mine, other)
    return jnp.stack([first, second], axis=1).reshape(-1, cols)


def reduce_weight(g):
    rows, cols = g.shape
    fsdp = lax.axis_size("fsdp")
    blocks = g.reshape(fsdp, 2, rows // (2 * fsdp), cols)
    core = lax.axis_index("core")
    mine = lax.dynamic_index_in_dim(blocks, core, axis=1, keepdims=False)
    other = lax.dynamic_index_in_dim(blocks, 1 - core, axis=1, keepdims=False)
    chip = mine + core_swap(other.astype(jnp.bfloat16)).astype(jnp.float32)
    part = lax.psum_scatter(chip.astype(jnp.bfloat16), "fsdp", scatter_dimension=0, tiled=True)
    part = lax.psum(part, ZAX).astype(jnp.float32)
    first, second = in_core_order(part, core_swap(part))
    return jnp.concatenate([first[0], second[0]], axis=0)


def shards(
    block_input,
    key_mask,
    slot_flags,
    norm1_gain,
    norm1_bias,
    qkv_weight,
    query_bias,
    value_bias,
    proj_weight,
    proj_bias,
    norm2_gain,
    norm2_bias,
    up_weight,
    up_bias,
    down_weight,
    down_bias,
    out_grad,
):
    f32, bf16 = jnp.float32, jnp.bfloat16
    pairs, part_rows, width = block_input.shape
    group = lax.axis_size("zl") * lax.axis_size("core")
    local_heads = HEADS // group
    slot_len = part_rows * group
    zh = lax.axis_index("zh")
    scale = HEAD ** (-0.5)

    vectors = (norm1_gain, norm1_bias, query_bias, value_bias, proj_bias, norm2_gain,
               norm2_bias, up_bias, down_bias)
    sizes = [v.shape[0] for v in vectors]
    packed = jnp.concatenate([v.astype(f32) for v in vectors])
    packed = lax.all_gather(packed, "fsdp", axis=0, tiled=False)
    full_vectors = []
    at = 0
    for n in sizes:
        full_vectors.append(packed[:, at : at + n].reshape(-1))
        at += n
    g1, b1, bq, bv, bproj, g2, b2, bup, bdown = full_vectors

    w_qkv = gather_weight(qkv_weight)
    w_proj = gather_weight(proj_weight)
    w_up = gather_weight(up_weight)
    w_down_t = gather_weight(down_weight.T)

    flags = slot_flags.astype(f32).reshape(pairs, 2)
    row_flags = lax.dynamic_index_in_dim(flags, zh, axis=1, keepdims=False)
    live = lax.dynamic_index_in_dim(key_mask.reshape(pairs, 2, -1), zh, axis=1, keepdims=False)
    mask_bias = (live.astype(f32) - 1.0) * 10000.0

    rows = block_input.reshape(pairs * part_rows, width).astype(f32)
    normed, norm_one_back = jax.vjp(layer_norm, rows, g1, b1)
    normed_low = normed.astype(bf16)
    mixed = jnp.dot(normed_low, w_qkv, preferred_element_type=f32)
    q = (mixed[:, :width] + bq).astype(bf16)
    k = mixed[:, width : 2 * width].astype(bf16)
    v = (mixed[:, 2 * width :] + bv).astype(bf16)
    qkv_tok = jnp.stack([q, k, v]).reshape(3, pairs, part_rows, width)
    qkv_heads = lax.all_to_all(qkv_tok, GROUP, split_axis=3, concat_axis=2, tiled=True)
    qkv_heads = qkv_heads.reshape(3, pairs, slot_len, local_heads, HEAD)
    qh, kh, vh = qkv_heads[0], qkv_heads[1], qkv_heads[2]

    scores = jnp.einsum("pqhd,pkhd->phqk", qh, kh, preferred_element_type=f32) * scale
    shifted = scores + mask_bias[:, None, None, :]
    row_max = jnp.max(shifted, axis=-1, keepdims=True)
    exp_terms = jnp.exp(shifted - row_max)
    probs = exp_terms / jnp.sum(exp_terms, axis=-1, keepdims=True)
    weights_low = probs.astype(bf16)
    attended = jnp.einsum("phqk,pkhd->pqhd", weights_low, vh, preferred_element_type=f32)
    attended = attended.astype(bf16).reshape(pairs, slot_len, local_heads * HEAD)
    merged = lax.all_to_all(attended, GROUP, split_axis=1, concat_axis=2, tiled=True)
    merged_rows = merged.reshape(pairs * part_rows, width)

    hidden = rows + jnp.dot(merged_rows, w_proj, preferred_element_type=f32) + bproj
    second, norm_two_back = jax.vjp(layer_norm, hidden, g2, b2)
    second_low = second.astype(bf16)
    gate_in = jnp.dot(second_low, w_up, preferred_element_type=f32) + bup
    active, gelu_back = jax.vjp(gelu_tanh, gate_in)
    active_low = active.astype(bf16)
    result = hidden + lax.dot_general(active_low, w_down_t, (((1,), (1,)), ((), ())), preferred_element_type=f32) + bdown
    row_flag_rows = jnp.repeat(row_flags, part_rows)[:, None]
    output = (result * row_flag_rows).astype(bf16).reshape(pairs, part_rows, width)

    grad_rows = out_grad.reshape(pairs * part_rows, width).astype(f32) * row_flag_rows
    grad_low = grad_rows.astype(bf16)
    down_weight_grad_t = jnp.dot(grad_low.T, active_low, preferred_element_type=f32)
    down_bias_grad = jnp.sum(grad_rows, axis=0)
    grad_active = jnp.dot(grad_low, w_down_t, preferred_element_type=f32)
    grad_gate = gelu_back(grad_active)[0].astype(bf16)
    up_weight_grad = jnp.dot(second_low.T, grad_gate, preferred_element_type=f32)
    up_bias_grad = jnp.sum(grad_gate.astype(f32), axis=0)
    grad_second = jnp.dot(grad_gate, w_up.T, preferred_element_type=f32)
    grad_hidden_norm, norm2_gain_grad, norm2_bias_grad = norm_two_back(grad_second)
    grad_hidden = grad_rows + grad_hidden_norm
    grad_branch = grad_hidden.astype(bf16)
    proj_weight_grad = jnp.dot(merged_rows.T, grad_branch, preferred_element_type=f32)
    proj_bias_grad = jnp.sum(grad_branch.astype(f32), axis=0)
    grad_merged = jnp.dot(grad_branch, w_proj.T, preferred_element_type=f32).astype(bf16)
    grad_heads = lax.all_to_all(
        grad_merged.reshape(pairs, part_rows, width), GROUP, split_axis=2, concat_axis=1, tiled=True
    ).reshape(pairs, slot_len, local_heads, HEAD)

    grad_probs = jnp.einsum("pqhd,pkhd->phqk", grad_heads, vh, preferred_element_type=f32)
    row_dot = jnp.sum(probs * grad_probs, axis=-1, keepdims=True)
    grad_scores = (probs * (grad_probs - row_dot)).astype(bf16)
    dq = (jnp.einsum("phqk,pkhd->pqhd", grad_scores, kh, preferred_element_type=f32) * scale).astype(bf16)
    dk = (jnp.einsum("phqk,pqhd->pkhd", grad_scores, qh, preferred_element_type=f32) * scale).astype(bf16)
    dv = jnp.einsum("phqk,pqhd->pkhd", weights_low, grad_heads, preferred_element_type=f32).astype(bf16)
    dqkv = jnp.stack([dq, dk, dv]).reshape(3, pairs, slot_len, local_heads * HEAD)
    dqkv_tok = lax.all_to_all(dqkv, GROUP, split_axis=2, concat_axis=3, tiled=True)
    dqkv_tok = dqkv_tok.reshape(3, pairs * part_rows, width)
    grad_mixed = jnp.concatenate([dqkv_tok[0], dqkv_tok[1], dqkv_tok[2]], axis=1)
    qkv_weight_grad = jnp.dot(normed_low.T, grad_mixed, preferred_element_type=f32)
    query_bias_grad = jnp.sum(dqkv_tok[0].astype(f32), axis=0)
    value_bias_grad = jnp.sum(dqkv_tok[2].astype(f32), axis=0)
    grad_normed = jnp.dot(grad_mixed, w_qkv.T, preferred_element_type=f32)
    grad_rows_norm, norm1_gain_grad, norm1_bias_grad = norm_one_back(grad_normed)
    input_grad = (grad_hidden + grad_rows_norm).reshape(pairs, part_rows, width)

    vec_grads = (norm1_gain_grad, norm1_bias_grad, query_bias_grad, value_bias_grad,
                 proj_bias_grad, norm2_gain_grad, norm2_bias_grad, up_bias_grad, down_bias_grad)
    fsdp = lax.axis_size("fsdp")
    stacked = jnp.concatenate([g.reshape(fsdp, -1) for g in vec_grads], axis=1)
    stacked = lax.psum_scatter(stacked, "fsdp", scatter_dimension=0, tiled=True)
    stacked = lax.psum(stacked, SEQ).reshape(-1)
    vec_out = []
    at = 0
    for g in vec_grads:
        n = g.shape[0] // fsdp
        vec_out.append(stacked[at : at + n])
        at += n
    (n1g, n1b, qb, vb, pb, n2g, n2b, ub, db) = vec_out

    down_g = reduce_weight(down_weight_grad_t).T
    up_g = reduce_weight(up_weight_grad)
    proj_g = reduce_weight(proj_weight_grad)
    qkv_g = reduce_weight(qkv_weight_grad)

    return (output, input_grad, n1g, n1b, qkv_g, qb, vb, proj_g, pb, n2g, n2b, up_g, ub, down_g, db)


def solution(mesh):
    seq_n = mesh.shape["seq"]
    fsdp_n = mesh.shape["fsdp"]
    devices = mesh.devices.reshape(2, seq_n // 4, 2, fsdp_n)
    inner = Mesh(devices, ("zh", "zl", "core", "fsdp"))
    tok = P("fsdp", SEQ, None)
    vec = P("fsdp")
    rows = P("fsdp", None)
    in_specs = (tok, rows, vec, vec, vec, rows, vec, vec, rows, vec, vec, vec, rows, vec,
                P(None, "fsdp"), vec, tok)
    out_specs = (tok, tok, vec, vec, rows, vec, vec, rows, vec, vec, vec, rows, vec,
                 P(None, "fsdp"), vec)
    return jax.shard_map(shards, mesh=inner, in_specs=in_specs, out_specs=out_specs, check_vma=False)
```

```python
import jax
import jax.numpy as jnp
from jax import lax
from jax.sharding import Mesh
from jax.sharding import PartitionSpec as P

HEADS = 16
HEAD = 72
epsilon = 1e-06

SEQ = ("zh", "zl", "core")
ZAX = ("zh", "zl")
GROUP = ("zl", "core")


def layer_norm(values, gain_vec, bias_vec):
    row_mean = jnp.mean(values, axis=-1, keepdims=True)
    centered = values - row_mean
    variance = jnp.mean(centered * centered, axis=-1, keepdims=True)
    return centered * lax.rsqrt(variance + epsilon) * gain_vec + bias_vec


def gelu_tanh(values):
    return (
        0.5
        * values
        * (1.0 + jnp.tanh(0.7978845608028654 * (values + 0.044715 * values * values * values)))
    )


def core_swap(x):
    return lax.ppermute(x, "core", [(0, 1), (1, 0)])


def in_core_order(mine, other):
    first = lax.axis_index("core") == 0
    return jnp.where(first, mine, other), jnp.where(first, other, mine)


def gather_weight(w):
    half = w.shape[0] // 2
    piece = lax.dynamic_slice_in_dim(w, lax.axis_index("core") * half, half, axis=0)
    return lax.all_gather(piece, ("fsdp", "core"), axis=0, tiled=True)


def reduce_weight(g):
    rows, cols = g.shape
    fsdp = lax.axis_size("fsdp")
    blocks = g.reshape(fsdp, 2, rows // (2 * fsdp), cols)
    core = lax.axis_index("core")
    mine = lax.dynamic_index_in_dim(blocks, core, axis=1, keepdims=False)
    other = lax.dynamic_index_in_dim(blocks, 1 - core, axis=1, keepdims=False)
    chip = mine + core_swap(other.astype(jnp.bfloat16)).astype(jnp.float32)
    part = lax.psum_scatter(chip.astype(jnp.bfloat16), "fsdp", scatter_dimension=0, tiled=True)
    part = lax.psum(part, ZAX).astype(jnp.float32)
    first, second = in_core_order(part, core_swap(part))
    return jnp.concatenate([first[0], second[0]], axis=0)


def shards(
    block_input,
    key_mask,
    slot_flags,
    norm1_gain,
    norm1_bias,
    qkv_weight,
    query_bias,
    value_bias,
    proj_weight,
    proj_bias,
    norm2_gain,
    norm2_bias,
    up_weight,
    up_bias,
    down_weight,
    down_bias,
    out_grad,
):
    f32, bf16 = jnp.float32, jnp.bfloat16
    pairs, part_rows, width = block_input.shape
    group = lax.axis_size("zl") * lax.axis_size("core")
    local_heads = HEADS // group
    slot_len = part_rows * group
    zh = lax.axis_index("zh")
    scale = HEAD ** (-0.5)

    vectors = (norm1_gain, norm1_bias, query_bias, value_bias, proj_bias, norm2_gain,
               norm2_bias, up_bias, down_bias)
    sizes = [v.shape[0] for v in vectors]
    packed = jnp.concatenate([v.astype(f32) for v in vectors])
    packed = lax.all_gather(packed, "fsdp", axis=0, tiled=False)
    full_vectors = []
    at = 0
    for n in sizes:
        full_vectors.append(packed[:, at : at + n].reshape(-1))
        at += n
    g1, b1, bq, bv, bproj, g2, b2, bup, bdown = full_vectors

    w_qkv = gather_weight(qkv_weight)
    w_proj = gather_weight(proj_weight)
    w_up = gather_weight(up_weight)
    w_down_t = gather_weight(down_weight.T)

    flags = slot_flags.astype(f32).reshape(pairs, 2)
    row_flags = lax.dynamic_index_in_dim(flags, zh, axis=1, keepdims=False)
    live = lax.dynamic_index_in_dim(key_mask.reshape(pairs, 2, -1), zh, axis=1, keepdims=False)
    mask_bias = (live.astype(f32) - 1.0) * 10000.0

    rows = block_input.reshape(pairs * part_rows, width).astype(f32)
    normed, norm_one_back = jax.vjp(layer_norm, rows, g1, b1)
    normed_low = normed.astype(bf16)
    mixed = jnp.dot(normed_low, w_qkv, preferred_element_type=f32)
    q = (mixed[:, :width] + bq).astype(bf16)
    k = mixed[:, width : 2 * width].astype(bf16)
    v = (mixed[:, 2 * width :] + bv).astype(bf16)
    qkv_tok = jnp.stack([q, k, v]).reshape(3, pairs, part_rows, width)
    qkv_heads = lax.all_to_all(qkv_tok, GROUP, split_axis=3, concat_axis=2, tiled=True)
    qkv_heads = qkv_heads.reshape(3, pairs, slot_len, local_heads, HEAD)
    qh, kh, vh = qkv_heads[0], qkv_heads[1], qkv_heads[2]

    scores = jnp.einsum("pqhd,pkhd->phqk", qh, kh, preferred_element_type=f32) * scale
    shifted = scores + mask_bias[:, None, None, :]
    row_max = jnp.max(shifted, axis=-1, keepdims=True)
    exp_terms = jnp.exp(shifted - row_max)
    probs = exp_terms / jnp.sum(exp_terms, axis=-1, keepdims=True)
    weights_low = probs.astype(bf16)
    attended = jnp.einsum("phqk,pkhd->pqhd", weights_low, vh, preferred_element_type=f32)
    attended = attended.astype(bf16).reshape(pairs, slot_len, local_heads * HEAD)
    merged = lax.all_to_all(attended, GROUP, split_axis=1, concat_axis=2, tiled=True)
    merged_rows = merged.reshape(pairs * part_rows, width)

    hidden = rows + jnp.dot(merged_rows, w_proj, preferred_element_type=f32) + bproj
    second, norm_two_back = jax.vjp(layer_norm, hidden, g2, b2)
    second_low = second.astype(bf16)
    gate_in = jnp.dot(second_low, w_up, preferred_element_type=f32) + bup
    active, gelu_back = jax.vjp(gelu_tanh, gate_in)
    active_low = active.astype(bf16)
    result = hidden + lax.dot_general(active_low, w_down_t, (((1,), (1,)), ((), ())), preferred_element_type=f32) + bdown
    row_flag_rows = jnp.repeat(row_flags, part_rows)[:, None]
    output = (result * row_flag_rows).astype(bf16).reshape(pairs, part_rows, width)

    grad_rows = out_grad.reshape(pairs * part_rows, width).astype(f32) * row_flag_rows
    grad_low = grad_rows.astype(bf16)
    down_weight_grad_t = jnp.dot(grad_low.T, active_low, preferred_element_type=f32)
    down_bias_grad = jnp.sum(grad_rows, axis=0)
    grad_active = jnp.dot(grad_low, w_down_t, preferred_element_type=f32)
    grad_gate = gelu_back(grad_active)[0].astype(bf16)
    up_weight_grad = jnp.dot(second_low.T, grad_gate, preferred_element_type=f32)
    up_bias_grad = jnp.sum(grad_gate.astype(f32), axis=0)
    grad_second = jnp.dot(grad_gate, w_up.T, preferred_element_type=f32)
    grad_hidden_norm, norm2_gain_grad, norm2_bias_grad = norm_two_back(grad_second)
    grad_hidden = grad_rows + grad_hidden_norm
    grad_branch = grad_hidden.astype(bf16)
    proj_weight_grad = jnp.dot(merged_rows.T, grad_branch, preferred_element_type=f32)
    proj_bias_grad = jnp.sum(grad_branch.astype(f32), axis=0)
    grad_merged = jnp.dot(grad_branch, w_proj.T, preferred_element_type=f32).astype(bf16)
    grad_heads = lax.all_to_all(
        grad_merged.reshape(pairs, part_rows, width), GROUP, split_axis=2, concat_axis=1, tiled=True
    ).reshape(pairs, slot_len, local_heads, HEAD)

    grad_probs = jnp.einsum("pqhd,pkhd->phqk", grad_heads, vh, preferred_element_type=f32)
    row_dot = jnp.sum(probs * grad_probs, axis=-1, keepdims=True)
    grad_scores = (probs * (grad_probs - row_dot)).astype(bf16)
    dq = (jnp.einsum("phqk,pkhd->pqhd", grad_scores, kh, preferred_element_type=f32) * scale).astype(bf16)
    dk = (jnp.einsum("phqk,pqhd->pkhd", grad_scores, qh, preferred_element_type=f32) * scale).astype(bf16)
    dv = jnp.einsum("phqk,pqhd->pkhd", weights_low, grad_heads, preferred_element_type=f32).astype(bf16)
    dqkv = jnp.stack([dq, dk, dv]).reshape(3, pairs, slot_len, local_heads * HEAD)
    dqkv_tok = lax.all_to_all(dqkv, GROUP, split_axis=2, concat_axis=3, tiled=True)
    dqkv_tok = dqkv_tok.reshape(3, pairs * part_rows, width)
    grad_mixed = jnp.concatenate([dqkv_tok[0], dqkv_tok[1], dqkv_tok[2]], axis=1)
    qkv_weight_grad = jnp.dot(normed_low.T, grad_mixed, preferred_element_type=f32)
    query_bias_grad = jnp.sum(dqkv_tok[0].astype(f32), axis=0)
    value_bias_grad = jnp.sum(dqkv_tok[2].astype(f32), axis=0)
    grad_normed = jnp.dot(grad_mixed, w_qkv.T, preferred_element_type=f32)
    grad_rows_norm, norm1_gain_grad, norm1_bias_grad = norm_one_back(grad_normed)
    input_grad = (grad_hidden + grad_rows_norm).reshape(pairs, part_rows, width)

    vec_grads = (norm1_gain_grad, norm1_bias_grad, query_bias_grad, value_bias_grad,
                 proj_bias_grad, norm2_gain_grad, norm2_bias_grad, up_bias_grad, down_bias_grad)
    fsdp = lax.axis_size("fsdp")
    stacked = jnp.concatenate([g.reshape(fsdp, -1) for g in vec_grads], axis=1)
    stacked = lax.psum_scatter(stacked, "fsdp", scatter_dimension=0, tiled=True)
    stacked = lax.psum(stacked, SEQ).reshape(-1)
    vec_out = []
    at = 0
    for g in vec_grads:
        n = g.shape[0] // fsdp
        vec_out.append(stacked[at : at + n])
        at += n
    (n1g, n1b, qb, vb, pb, n2g, n2b, ub, db) = vec_out

    down_g = reduce_weight(down_weight_grad_t)
    up_weight_grad, down_g = lax.optimization_barrier((up_weight_grad, down_g))
    up_g = reduce_weight(up_weight_grad)
    proj_weight_grad, up_g = lax.optimization_barrier((proj_weight_grad, up_g))
    proj_g = reduce_weight(proj_weight_grad)
    qkv_weight_grad, proj_g = lax.optimization_barrier((qkv_weight_grad, proj_g))
    qkv_g = reduce_weight(qkv_weight_grad)
    down_g = down_g.T

    return (output, input_grad, n1g, n1b, qkv_g, qb, vb, proj_g, pb, n2g, n2b, up_g, ub, down_g, db)


def solution(mesh):
    seq_n = mesh.shape["seq"]
    fsdp_n = mesh.shape["fsdp"]
    devices = mesh.devices.reshape(2, seq_n // 4, 2, fsdp_n)
    inner = Mesh(devices, ("zh", "zl", "core", "fsdp"))
    tok = P("fsdp", SEQ, None)
    vec = P("fsdp")
    rows = P("fsdp", None)
    in_specs = (tok, rows, vec, vec, vec, rows, vec, vec, rows, vec, vec, vec, rows, vec,
                P(None, "fsdp"), vec, tok)
    out_specs = (tok, tok, vec, vec, rows, vec, vec, rows, vec, vec, vec, rows, vec,
                 P(None, "fsdp"), vec)
    return jax.shard_map(shards, mesh=inner, in_specs=in_specs, out_specs=out_specs, check_vma=False)
```

```python
import jax
import jax.numpy as jnp
from jax import lax
from jax.sharding import Mesh
from jax.sharding import PartitionSpec as P

HEADS = 16
HEAD = 72
epsilon = 1e-06

SEQ = ("zh", "zl", "core")
ZAX = ("zh", "zl")
GROUP = ("zl", "core")


def layer_norm(values, gain_vec, bias_vec):
    row_mean = jnp.mean(values, axis=-1, keepdims=True)
    centered = values - row_mean
    variance = jnp.mean(centered * centered, axis=-1, keepdims=True)
    return centered * lax.rsqrt(variance + epsilon) * gain_vec + bias_vec


def gelu_tanh(values):
    return (
        0.5
        * values
        * (1.0 + jnp.tanh(0.7978845608028654 * (values + 0.044715 * values * values * values)))
    )


def core_swap(x):
    return lax.ppermute(x, "core", [(0, 1), (1, 0)])


def in_core_order(mine, other):
    first = lax.axis_index("core") == 0
    return jnp.where(first, mine, other), jnp.where(first, other, mine)


def gather_weight(w):
    half = w.shape[0] // 2
    piece = lax.dynamic_slice_in_dim(w, lax.axis_index("core") * half, half, axis=0)
    return lax.all_gather(piece, ("fsdp", "core"), axis=0, tiled=True)


def reduce_weight(g):
    rows, cols = g.shape
    fsdp = lax.axis_size("fsdp")
    blocks = g.reshape(fsdp, 2, rows // (2 * fsdp), cols)
    core = lax.axis_index("core")
    mine = lax.dynamic_index_in_dim(blocks, core, axis=1, keepdims=False)
    other = lax.dynamic_index_in_dim(blocks, 1 - core, axis=1, keepdims=False)
    chip = mine + core_swap(other.astype(jnp.bfloat16)).astype(jnp.float32)
    part = lax.psum_scatter(chip.astype(jnp.bfloat16), "fsdp", scatter_dimension=0, tiled=True)
    part = lax.psum(part, ZAX).astype(jnp.float32)
    first, second = in_core_order(part, core_swap(part))
    return jnp.concatenate([first[0], second[0]], axis=0)


def shards(
    block_input,
    key_mask,
    slot_flags,
    norm1_gain,
    norm1_bias,
    qkv_weight,
    query_bias,
    value_bias,
    proj_weight,
    proj_bias,
    norm2_gain,
    norm2_bias,
    up_weight,
    up_bias,
    down_weight,
    down_bias,
    out_grad,
):
    f32, bf16 = jnp.float32, jnp.bfloat16
    pairs, part_rows, width = block_input.shape
    group = lax.axis_size("zl") * lax.axis_size("core")
    local_heads = HEADS // group
    slot_len = part_rows * group
    zh = lax.axis_index("zh")
    scale = HEAD ** (-0.5)

    vectors = (norm1_gain, norm1_bias, query_bias, value_bias, proj_bias, norm2_gain,
               norm2_bias, up_bias, down_bias)
    sizes = [v.shape[0] for v in vectors]
    packed = jnp.concatenate([v.astype(f32) for v in vectors])
    packed = lax.all_gather(packed, "fsdp", axis=0, tiled=False)
    full_vectors = []
    at = 0
    for n in sizes:
        full_vectors.append(packed[:, at : at + n].reshape(-1))
        at += n
    g1, b1, bq, bv, bproj, g2, b2, bup, bdown = full_vectors

    w_qkv = gather_weight(qkv_weight)
    w_proj = gather_weight(proj_weight)
    w_up = gather_weight(up_weight)
    w_down_t = gather_weight(down_weight.T)

    flags = slot_flags.astype(f32).reshape(pairs, 2)
    row_flags = lax.dynamic_index_in_dim(flags, zh, axis=1, keepdims=False)
    live = lax.dynamic_index_in_dim(key_mask.reshape(pairs, 2, -1), zh, axis=1, keepdims=False)
    mask_bias = (live.astype(f32) - 1.0) * 10000.0

    rows = block_input.reshape(pairs * part_rows, width).astype(f32)
    normed, norm_one_back = jax.vjp(layer_norm, rows, g1, b1)
    normed_low = normed.astype(bf16)
    mixed = jnp.dot(normed_low, w_qkv, preferred_element_type=f32)
    q = (mixed[:, :width] + bq).astype(bf16)
    k = mixed[:, width : 2 * width].astype(bf16)
    v = (mixed[:, 2 * width :] + bv).astype(bf16)
    qkv_tok = jnp.stack([q, k, v]).reshape(3, pairs, part_rows, width)
    qkv_heads = lax.all_to_all(qkv_tok, GROUP, split_axis=3, concat_axis=2, tiled=True)
    qkv_heads = qkv_heads.reshape(3, pairs, slot_len, local_heads, HEAD)
    qh, kh, vh = qkv_heads[0], qkv_heads[1], qkv_heads[2]

    scores = jnp.einsum("pqhd,pkhd->phqk", qh, kh, preferred_element_type=f32) * scale
    shifted = scores + mask_bias[:, None, None, :]
    row_max = jnp.max(shifted, axis=-1, keepdims=True)
    exp_terms = jnp.exp(shifted - row_max)
    probs = exp_terms / jnp.sum(exp_terms, axis=-1, keepdims=True)
    weights_low = probs.astype(bf16)
    attended = jnp.einsum("phqk,pkhd->pqhd", weights_low, vh, preferred_element_type=f32)
    attended = attended.astype(bf16).reshape(pairs, slot_len, local_heads * HEAD)
    merged = lax.all_to_all(attended, GROUP, split_axis=1, concat_axis=2, tiled=True)
    merged_rows = merged.reshape(pairs * part_rows, width)

    hidden = rows + jnp.dot(merged_rows, w_proj, preferred_element_type=f32) + bproj
    second, norm_two_back = jax.vjp(layer_norm, hidden, g2, b2)
    second_low = second.astype(bf16)
    gate_in = jnp.dot(second_low, w_up, preferred_element_type=f32) + bup
    active, gelu_back = jax.vjp(gelu_tanh, gate_in)
    active_low = active.astype(bf16)
    result = hidden + lax.dot_general(active_low, w_down_t, (((1,), (1,)), ((), ())), preferred_element_type=f32) + bdown
    row_flag_rows = jnp.repeat(row_flags, part_rows)[:, None]
    output = (result * row_flag_rows).astype(bf16).reshape(pairs, part_rows, width)

    out_grad, output = lax.optimization_barrier((out_grad, output))
    grad_rows = out_grad.reshape(pairs * part_rows, width).astype(f32) * row_flag_rows
    grad_low = grad_rows.astype(bf16)
    down_weight_grad_t = jnp.dot(grad_low.T, active_low, preferred_element_type=f32)
    down_bias_grad = jnp.sum(grad_rows, axis=0)
    grad_active = jnp.dot(grad_low, w_down_t, preferred_element_type=f32)
    grad_gate = gelu_back(grad_active)[0].astype(bf16)
    up_weight_grad = jnp.dot(second_low.T, grad_gate, preferred_element_type=f32)
    up_bias_grad = jnp.sum(grad_gate.astype(f32), axis=0)
    grad_second = jnp.dot(grad_gate, w_up.T, preferred_element_type=f32)
    grad_hidden_norm, norm2_gain_grad, norm2_bias_grad = norm_two_back(grad_second)
    grad_hidden = grad_rows + grad_hidden_norm
    grad_branch = grad_hidden.astype(bf16)
    proj_weight_grad = jnp.dot(merged_rows.T, grad_branch, preferred_element_type=f32)
    proj_bias_grad = jnp.sum(grad_branch.astype(f32), axis=0)
    grad_merged = jnp.dot(grad_branch, w_proj.T, preferred_element_type=f32).astype(bf16)
    grad_heads = lax.all_to_all(
        grad_merged.reshape(pairs, part_rows, width), GROUP, split_axis=2, concat_axis=1, tiled=True
    ).reshape(pairs, slot_len, local_heads, HEAD)

    grad_probs = jnp.einsum("pqhd,pkhd->phqk", grad_heads, vh, preferred_element_type=f32)
    row_dot = jnp.sum(probs * grad_probs, axis=-1, keepdims=True)
    grad_scores = (probs * (grad_probs - row_dot)).astype(bf16)
    dq = (jnp.einsum("phqk,pkhd->pqhd", grad_scores, kh, preferred_element_type=f32) * scale).astype(bf16)
    dk = (jnp.einsum("phqk,pqhd->pkhd", grad_scores, qh, preferred_element_type=f32) * scale).astype(bf16)
    dv = jnp.einsum("phqk,pqhd->pkhd", weights_low, grad_heads, preferred_element_type=f32).astype(bf16)
    dqkv = jnp.stack([dq, dk, dv]).reshape(3, pairs, slot_len, local_heads * HEAD)
    dqkv_tok = lax.all_to_all(dqkv, GROUP, split_axis=2, concat_axis=3, tiled=True)
    dqkv_tok = dqkv_tok.reshape(3, pairs * part_rows, width)
    grad_mixed = jnp.concatenate([dqkv_tok[0], dqkv_tok[1], dqkv_tok[2]], axis=1)
    qkv_weight_grad = jnp.dot(normed_low.T, grad_mixed, preferred_element_type=f32)
    query_bias_grad = jnp.sum(dqkv_tok[0].astype(f32), axis=0)
    value_bias_grad = jnp.sum(dqkv_tok[2].astype(f32), axis=0)
    grad_normed = jnp.dot(grad_mixed, w_qkv.T, preferred_element_type=f32)
    grad_rows_norm, norm1_gain_grad, norm1_bias_grad = norm_one_back(grad_normed)
    input_grad = (grad_hidden + grad_rows_norm).reshape(pairs, part_rows, width)

    vec_grads = (norm1_gain_grad, norm1_bias_grad, query_bias_grad, value_bias_grad,
                 proj_bias_grad, norm2_gain_grad, norm2_bias_grad, up_bias_grad, down_bias_grad)
    fsdp = lax.axis_size("fsdp")
    stacked = jnp.concatenate([g.reshape(fsdp, -1) for g in vec_grads], axis=1)
    stacked = lax.psum_scatter(stacked, "fsdp", scatter_dimension=0, tiled=True)
    stacked = lax.psum(stacked, SEQ).reshape(-1)
    vec_out = []
    at = 0
    for g in vec_grads:
        n = g.shape[0] // fsdp
        vec_out.append(stacked[at : at + n])
        at += n
    (n1g, n1b, qb, vb, pb, n2g, n2b, ub, db) = vec_out

    down_g = reduce_weight(down_weight_grad_t)
    up_weight_grad, down_g = lax.optimization_barrier((up_weight_grad, down_g))
    up_g = reduce_weight(up_weight_grad)
    proj_weight_grad, up_g = lax.optimization_barrier((proj_weight_grad, up_g))
    proj_g = reduce_weight(proj_weight_grad)
    qkv_weight_grad, proj_g = lax.optimization_barrier((qkv_weight_grad, proj_g))
    qkv_g = reduce_weight(qkv_weight_grad)
    down_g = down_g.T

    return (output, input_grad, n1g, n1b, qkv_g, qb, vb, proj_g, pb, n2g, n2b, up_g, ub, down_g, db)


def solution(mesh):
    seq_n = mesh.shape["seq"]
    fsdp_n = mesh.shape["fsdp"]
    devices = mesh.devices.reshape(2, seq_n // 4, 2, fsdp_n)
    inner = Mesh(devices, ("zh", "zl", "core", "fsdp"))
    tok = P("fsdp", SEQ, None)
    vec = P("fsdp")
    rows = P("fsdp", None)
    in_specs = (tok, rows, vec, vec, vec, rows, vec, vec, rows, vec, vec, vec, rows, vec,
                P(None, "fsdp"), vec, tok)
    out_specs = (tok, tok, vec, vec, rows, vec, vec, rows, vec, vec, vec, rows, vec,
                 P(None, "fsdp"), vec)
    return jax.shard_map(shards, mesh=inner, in_specs=in_specs, out_specs=out_specs, check_vma=False)
```
